512 devices in a mesh: rows: 512 (over z, y, x, core).
Axes of the slice: x: 4, y: 8, z: 8, core: 2. Of those that a mesh axis runs over, the one named last changes fastest.
Arguments:
- adj_diag: int32 [8192, 512], P('rows'), may hold values from -2147483648 to 2147483647
- adj_right: int32 [8192, 512], P('rows'), may hold values from -2147483648 to 2147483647
- alive_diag: int32 [8192, 512], P('rows'), may hold values from -2147483648 to 2147483647
- alive_right: int32 [8192, 512], P('rows'), may hold values from -2147483648 to 2147483647
- truss_k: int32 [1], replicated, may hold values from 130 to 193
Outputs:
- support_field: float32 [262144, 1024], P('rows')
- removed_counts: int32 [3], replicated
The draws below stay inside these ranges and needn't reach their ends.
All inputs are finite; a program needn't handle non-finite values.
Results may differ from the reference program's by a relative error of at most 0.0003.
Values may be sent and summed in bfloat16 or wider, within the bound.
No kernel may reach another device: no remote copies, remote signals or barrier semaphores. Data moves between devices by JAX's collectives and lax.ppermute only.
A program may use at most 64 MiB of HBM per device.

```python
import jax
import jax.numpy as jnp
from jax import lax

TILE = 512
ITERS = 3
NVERT = 262144


def vertex_levels(key, block):
    base_key = jax.random.fold_in(jax.random.fold_in(key, 7001), block)
    size_key, order_key, level_key = jax.random.split(base_key, 3)
    core_count = jax.random.randint(size_key, (), TILE // 4, 3 * TILE // 8 + 1, dtype=jnp.int32)
    order = jax.random.permutation(order_key, TILE)
    is_core = order < core_count
    levels = jax.random.randint(level_key, (TILE,), 2, 16, dtype=jnp.int32)
    return (jnp.where(is_core, jnp.int32(16), levels), is_core)


def pack_bits(tile_bits):
    shifts = jnp.arange(32, dtype=jnp.int32)
    sectioned = tile_bits.reshape(TILE // 32, 32, TILE)
    return jnp.sum(sectioned << shifts[None, :, None], axis=1, dtype=jnp.int32)


def draw_bits(key, salt, offset, alive_kind):
    blocks = NVERT // TILE

    def one_block(block):
        row_levels, row_core = vertex_levels(key, block)
        col_levels, col_core = vertex_levels(key, (block + offset) % blocks)
        edge_key = jax.random.fold_in(jax.random.fold_in(key, salt), block)
        if alive_kind:
            chance = jax.random.randint(edge_key, (TILE, TILE), 0, 8, dtype=jnp.int32)
            both_core = row_core[:, None] & col_core[None, :]
            tile_bits = jnp.where(both_core, jnp.int32(1), (chance < 7).astype(jnp.int32))
        else:
            chance = jax.random.randint(edge_key, (TILE, TILE), 0, 256, dtype=jnp.int32)
            tile_bits = (chance < row_levels[:, None] * col_levels[None, :]).astype(jnp.int32)
        return pack_bits(tile_bits)
    packed = lax.map(one_block, jnp.arange(blocks, dtype=jnp.int32))
    return packed.reshape(NVERT // 32, TILE)


def draw_adj_diag(key, part):
    return draw_bits(key, 101, 0, False)


def draw_adj_right(key, part):
    return draw_bits(key, 102, 1, False)


def draw_alive_diag(key, part):
    return draw_bits(key, 103, 0, True)


def draw_alive_right(key, part):
    return draw_bits(key, 104, 1, True)


def setup_inputs(seed: int = 0) -> dict:
    seeds = jax.random.split(jax.random.key(seed), 6)
    adj_diag = draw_adj_diag(jax.random.fold_in(seeds[5], 71), 0)
    adj_right = draw_adj_right(jax.random.fold_in(seeds[5], 71), 0)
    alive_diag = draw_alive_diag(jax.random.fold_in(seeds[5], 71), 0)
    alive_right = draw_alive_right(jax.random.fold_in(seeds[5], 71), 0)
    truss_k = jax.random.randint(seeds[4], (1,), TILE // 4 + 2, 3 * TILE // 8 + 2).astype(jnp.int32)
    return {"adj_diag": adj_diag, "adj_right": adj_right, "alive_diag": alive_diag, "alive_right": alive_right, "truss_k": truss_k}


def unpack_tiles(packed, blocks, tile):
    shifts = jnp.arange(32, dtype=jnp.int32)
    sectioned = packed.reshape(blocks, tile // 32, tile)
    tile_bits = (sectioned[:, :, None, :] >> shifts[None, None, :, None]) & 1
    return tile_bits.reshape(blocks, tile, tile)


def tile_support(pieces):
    within, across, prev_across, next_within = pieces
    inside = lax.dot_general(prev_across, prev_across, (((0,), (0,)), ((), ())), preferred_element_type=jnp.float32)
    inside = inside + jnp.dot(within, within, preferred_element_type=jnp.float32)
    inside = inside + lax.dot_general(across, across, (((1,), (1,)), ((), ())), preferred_element_type=jnp.float32)
    between = jnp.dot(within, across, preferred_element_type=jnp.float32)
    between = between + jnp.dot(across, next_within, preferred_element_type=jnp.float32)
    return inside, between


def reference(adj_diag, adj_right, alive_diag, alive_right, truss_k):
    blocks = NVERT // TILE
    upper_half = jnp.triu(unpack_tiles(adj_diag & alive_diag, blocks, TILE), 1)
    within = (upper_half + jnp.swapaxes(upper_half, 1, 2)).astype(jnp.bfloat16)
    across = unpack_tiles(adj_right & alive_right, blocks, TILE).astype(jnp.bfloat16)
    thresh = (truss_k[0] - 2).astype(jnp.float32)
    counts = []
    for step in range(ITERS):
        prev_across = jnp.roll(across, 1, axis=0)
        next_within = jnp.roll(within, -1, axis=0)
        inside, between = lax.map(tile_support, (within, across, prev_across, next_within))
        new_within = jnp.where(inside >= thresh, within, jnp.zeros_like(within))
        new_across = jnp.where(between >= thresh, across, jnp.zeros_like(across))
        lost_within = jnp.sum((within - new_within).astype(jnp.int32)) // 2
        lost_across = jnp.sum((across - new_across).astype(jnp.int32))
        counts.append(lost_within + lost_across)
        within, across = new_within, new_across
    support = jnp.concatenate([inside * within.astype(jnp.float32), between * across.astype(jnp.float32)], axis=2)
    return support.reshape(NVERT, 2 * TILE), jnp.stack(counts).astype(jnp.int32)
```

```python
import jax
import jax.numpy as jnp
from jax import lax
from jax.experimental import pallas as pl
from jax.experimental.pallas import tpu as pltpu
from jax.sharding import Mesh
from jax.sharding import PartitionSpec as P

ITERS = 3
TILE = 512
WORDS = TILE // 32
SPAN = 5
ROWS = ("z", "y", "x", "core")
KIND = jnp.float8_e4m3fn


def unpack_words(words):
    shifts = lax.broadcasted_iota(jnp.int32, (WORDS, 32, TILE), 1)
    spread = jnp.broadcast_to(words[:, None, :], (WORDS, 32, TILE))
    bits = (spread >> shifts) & 1
    return bits.reshape(TILE, TILE).astype(jnp.float32)


def peel_kernel(core_ref, thresh_ref, far_ref, chip_ref, near_ref, out_ref, count_ref, band_a, band_b):
    first = core_ref[0] == 0
    thresh = thresh_ref[0].astype(jnp.float32)

    def block(ref, p, q):
        return ref.at[p * TILE : (p + 1) * TILE, q * TILE : (q + 1) * TILE]

    def piece(index):
        def rows(parts):
            at = index * WORDS
            for ref in parts:
                if at < ref.shape[0]:
                    return ref[at : at + WORDS, :]
                at -= ref.shape[0]

        left = rows((far_ref, chip_ref, near_ref))
        right = rows((near_ref, chip_ref, far_ref))
        return jnp.where(first, left, right)

    row_ids = lax.broadcasted_iota(jnp.int32, (TILE, TILE), 0)
    col_ids = lax.broadcasted_iota(jnp.int32, (TILE, TILE), 1)
    for index in range(8):
        tile = unpack_words(piece(index))
        p = (index + 1) // 2
        if index % 2:
            upper = jnp.where(col_ids > row_ids, tile, 0.0)
            block(band_a, p, p)[...] = (upper + upper.T).astype(KIND)
        else:
            block(band_a, p, p + 1)[...] = tile.astype(KIND)
            block(band_a, p + 1, p)[...] = tile.T.astype(KIND)

    def total(ref, p, q):
        ones = jnp.ones((32, TILE), KIND)
        sums = jnp.dot(ones, block(ref, p, q)[...], preferred_element_type=jnp.float32)
        return jnp.sum(sums[:8], axis=1, keepdims=True)

    def support(ref, p, q):
        lo = min(p, q) - (p == q)
        hi = max(p, q) + (p == q)
        lhs = ref[p * TILE : (p + 1) * TILE, lo * TILE : (hi + 1) * TILE]
        rhs = ref[lo * TILE : (hi + 1) * TILE, q * TILE : (q + 1) * TILE]
        return jnp.dot(lhs, rhs, preferred_element_type=jnp.float32)

    old, new = band_a, band_b
    sums = [(total(old, 2, 2), total(old, 2, 3))]
    for step in range(ITERS):
        for index in range(1 + step, 7 - step):
            p = (index + 1) // 2
            q = p + (index + 1) % 2
            counts = support(old, p, q)
            mask = block(old, p, q)[...].astype(jnp.float32)
            kept = jnp.where(counts >= thresh, mask, 0.0)
            block(new, p, q)[...] = kept.astype(KIND)
            if p != q and step < ITERS - 1:
                block(new, q, p)[...] = kept.T.astype(KIND)
            if step == ITERS - 1:
                out_ref[:, (q - 2) * TILE : (q - 1) * TILE] = counts * kept
        sums.append((total(new, 2, 2), total(new, 2, 3)))
        old, new = new, old

    lane = lax.broadcasted_iota(jnp.int32, (8, 128), 1)
    removed = jnp.zeros((8, 128), jnp.float32)
    for step in range(ITERS):
        within = (sums[step][0] - sums[step + 1][0]) * 0.5
        across = sums[step][1] - sums[step + 1][1]
        removed = jnp.where(lane == step, within + across, removed)
    count_ref[...] = removed.astype(jnp.int32)


def peel(core, thresh, far, chip, near):
    vmem = pl.BlockSpec(memory_space=pltpu.VMEM)
    smem = pl.BlockSpec(memory_space=pltpu.SMEM)
    return pl.pallas_call(
        peel_kernel,
        out_shape=(
            jax.ShapeDtypeStruct((TILE, 2 * TILE), jnp.float32),
            jax.ShapeDtypeStruct((8, 128), jnp.int32),
        ),
        in_specs=[smem, smem, vmem, vmem, vmem],
        out_specs=(vmem, vmem),
        scratch_shapes=[
            pltpu.VMEM((SPAN * TILE, SPAN * TILE), KIND),
            pltpu.VMEM((SPAN * TILE, SPAN * TILE), KIND),
        ],
        compiler_params=pltpu.CompilerParams(vmem_limit_bytes=60 * 1024 * 1024),
    )(core, thresh, far, chip, near)


def gather_sum(values, axes, members):
    spread = jnp.broadcast_to(values[None], (members,) + values.shape)
    return jnp.sum(lax.all_to_all(spread, axes, 0, 0), axis=0)


def on_device(adj_diag, adj_right, alive_diag, alive_right, truss_k):
    count = lax.axis_size(ROWS)
    core = lax.axis_index("core")
    within = adj_diag & alive_diag
    across = adj_right & alive_right
    near = lax.ppermute(
        jnp.where(core == 0, within, across),
        ROWS,
        [(i, (i + 2 if i % 2 else i - 2) % count) for i in range(count)],
    )
    chip = lax.all_gather(jnp.concatenate([within, across], axis=0), "core", tiled=True)
    far = lax.ppermute(
        jnp.where(core == 0, chip[: 3 * WORDS], chip[WORDS:]),
        ROWS,
        [(i, (i + 1 if i % 2 else i - 1) % count) for i in range(count)],
    )
    support, removed = peel(core.reshape(1), truss_k - 2, far, chip, near)
    removed = gather_sum(removed[0, :ITERS], ("y", "core"), 16)
    removed = gather_sum(removed, ("z", "x"), 32)
    return (support, removed)


def solution(mesh):
    split = Mesh(mesh.devices.reshape(8, 8, 4, 2), ROWS)
    placed = (P(ROWS, None), P(ROWS, None), P(ROWS, None), P(ROWS, None), P())
    return jax.shard_map(
        on_device, mesh=split, in_specs=placed, out_specs=(P(ROWS, None), P()), check_vma=False
    )
```

```python
import functools

import jax
import jax.numpy as jnp
from jax import lax
from jax.experimental import pallas as pl
from jax.experimental.pallas import tpu as pltpu
from jax.sharding import Mesh
from jax.sharding import PartitionSpec as P

ITERS = 3
TILE = 512
HALF = TILE // 2
WORDS = TILE // 32
SIDE = 128
ROWS = ("z", "y", "x", "core")
FIRST = ("y", "core")
SECOND = ("z", "x")
KIND = jnp.float8_e4m3fn
WIDE = jnp.bfloat16
MIB = 1024 * 1024


def unpack(words):
    rows, width = words.shape
    shifts = lax.broadcasted_iota(jnp.int32, (rows, 32, width), 1)
    spread = jnp.broadcast_to(words[:, None, :], (rows, 32, width))
    return ((spread >> shifts) & 1).reshape(rows * 32, width).astype(jnp.float32)


def fill_within(words, ref):
    row_ids = lax.broadcasted_iota(jnp.int32, (SIDE, SIDE), 0)
    col_ids = lax.broadcasted_iota(jnp.int32, (SIDE, SIDE), 1)
    for at in range(0, TILE, SIDE):
        stripe = unpack(words[at // 32 : (at + SIDE) // 32, at:])
        corner = jnp.where(col_ids > row_ids, stripe[:, :SIDE], 0.0)
        flipped = corner.astype(KIND).T.astype(jnp.float32)
        ref[at : at + SIDE, at : at + SIDE] = (corner + flipped).astype(KIND)
        if at + SIDE < TILE:
            rest = stripe[:, SIDE:].astype(KIND)
            ref[at : at + SIDE, at + SIDE :] = rest
            ref[at + SIDE :, at : at + SIDE] = rest.T


def fill_across(words, ref, ref_t):
    tile = unpack(words).astype(KIND)
    ref[...] = tile
    ref_t[...] = tile.T


def times(lhs, rhs):
    return jnp.dot(lhs, rhs, preferred_element_type=jnp.float32)


def inside(left, left_t, here, right, right_t, rows, cols):
    return (
        times(left_t[rows, :], left[:, cols])
        + times(here[rows, :], here[:, cols])
        + times(right[rows, :], right_t[:, cols])
    )


def between(left, here, right, rows):
    return times(left[rows, :], here[...]) + times(here[rows, :], right[...])


def keep(counts, old, thresh):
    return jnp.where(counts.astype(WIDE) >= thresh, old.astype(WIDE), jnp.zeros((), WIDE)).astype(KIND)


TOP, LOW = slice(0, HALF), slice(HALF, TILE)
ALL = slice(0, TILE)


def peel_within(left, left_t, here, right, right_t, thresh, new):
    kept = keep(inside(left, left_t, here, right, right_t, TOP, ALL), here[TOP, :], thresh)
    new[TOP, :] = kept
    new[LOW, TOP] = kept[:, HALF:].T
    new[LOW, LOW] = keep(inside(left, left_t, here, right, right_t, LOW, LOW), here[LOW, LOW], thresh)


def peel_across(left, here, right, thresh, new, new_t):
    for rows in (TOP, LOW):
        kept = keep(between(left, here, right, rows), here[rows, :], thresh)
        new[rows, :] = kept
        new_t[:, rows] = kept.T


def chip_kernel(thresh_ref, chip_ref, tiles_ref):
    thresh = thresh_ref[0].astype(jnp.float32).astype(WIDE)
    w0, a0, a0_t, w1, a1, a1_t, new_a0, new_a0_t, new_w1 = (tiles_ref.at[i] for i in range(9))
    fill_within(chip_ref[:WORDS, :], w0)
    fill_across(chip_ref[WORDS : 2 * WORDS, :], a0, a0_t)
    fill_within(chip_ref[2 * WORDS : 3 * WORDS, :], w1)
    fill_across(chip_ref[3 * WORDS :, :], a1, a1_t)
    peel_across(w0, a0, w1, thresh, new_a0, new_a0_t)
    peel_within(a0, a0_t, w1, a1, a1_t, thresh, new_w1)


def edges(ref):
    tile = ref[...].astype(WIDE)
    parts = [tile[at : at + 32, :] for at in range(0, TILE, 32)]
    while len(parts) > 1:
        parts = [parts[i] + parts[i + 1] for i in range(0, len(parts), 2)]
    return parts[0].astype(jnp.float32)


def peel_kernel(core_ref, thresh_ref, far_ref, near_ref, chip_ref, out_ref, count_ref, pool):
    def body(core):
        level = thresh_ref[0].astype(jnp.float32)
        thresh = level.astype(WIDE)
        slots = iter(range(pool.shape[0]))

        def fresh():
            return pool.at[next(slots)]

        w0, a0, a0_t, w1, a1, a1_t, new_a0, new_a0_t, new_w1 = (chip_ref.at[i] for i in range(9))
        shift = 3 - 2 * core
        now = {shift: (w0,), shift + 1: (a0, a0_t), shift + 2: (w1,), shift + 3: (a1, a1_t)}
        new = {shift + 1: (new_a0, new_a0_t), shift + 2: (new_w1,)}

        def words(index):
            at = index - 5 * core
            if 0 <= at < 3:
                return far_ref[at * WORDS : (at + 1) * WORDS, :]
            return near_ref[...]

        for index in range(8):
            if index not in now and index % 2:
                now[index] = (fresh(),)
                fill_within(words(index), *now[index])
            elif index not in now:
                now[index] = (fresh(), fresh())
                fill_across(words(index), *now[index])

        total = [edges(now[3][0]) * 0.5 + edges(now[4][0])]
        for step in range(ITERS - 1):
            for index in range(1 + step, 7 - step):
                if index in new:
                    continue
                left, here, right = now[index - 1], now[index], now[index + 1]
                if index % 2:
                    new[index] = (fresh(),)
                    peel_within(*left, *here, *right, thresh, *new[index])
                else:
                    new[index] = (fresh(), fresh())
                    peel_across(left[0], here[0], right[0], thresh, *new[index])
            now, new = new, {}
            total.append(edges(now[3][0]) * 0.5 + edges(now[4][0]))

        last = jnp.zeros((8, TILE), jnp.float32)
        for rows in (TOP, LOW):
            counts = inside(*now[2], *now[3], *now[4], rows, ALL)
            kept = jnp.where(counts >= level, now[3][0][rows, :].astype(jnp.float32), 0.0)
            out_ref[rows, :TILE] = counts * kept
            last = last + 0.5 * jnp.sum(kept.reshape(HALF // 8, 8, TILE), axis=0)
            counts = between(*now[3], now[4][0], *now[5], rows)
            kept = jnp.where(counts >= level, now[4][0][rows, :].astype(jnp.float32), 0.0)
            out_ref[rows, TILE:] = counts * kept
            last = last + jnp.sum(kept.reshape(HALF // 8, 8, TILE), axis=0)

        sums = [jnp.sum(part) for part in total] + [jnp.sum(last)]
        lane = lax.broadcasted_iota(jnp.int32, count_ref.shape, count_ref.ndim - 1)
        removed = jnp.zeros(count_ref.shape, jnp.float32)
        for step in range(ITERS):
            removed = jnp.where(lane == step, sums[step] - sums[step + 1], removed)
        count_ref[...] = removed.astype(jnp.int32)

    for core in range(2):
        pl.when(core_ref[0] == core)(functools.partial(body, core))


VMEM = pl.BlockSpec(memory_space=pltpu.VMEM)
SMEM = pl.BlockSpec(memory_space=pltpu.SMEM)


def chip_tiles(thresh, chip):
    return pl.pallas_call(
        chip_kernel,
        out_shape=jax.ShapeDtypeStruct((9, TILE, TILE), KIND),
        in_specs=[SMEM, VMEM],
        out_specs=VMEM,
        compiler_params=pltpu.CompilerParams(vmem_limit_bytes=8 * MIB),
        cost_estimate=pl.CostEstimate(flops=10 * TILE**3, bytes_accessed=0, transcendentals=0),
    )(thresh, chip)


def peel(core, thresh, far, near, tiles):
    return pl.pallas_call(
        peel_kernel,
        out_shape=(
            pltpu.VMEM((TILE, 2 * TILE), jnp.float32),
            jax.ShapeDtypeStruct((16, 1, 128), jnp.int32),
        ),
        in_specs=[SMEM, SMEM, VMEM, VMEM, VMEM],
        out_specs=(VMEM, VMEM),
        scratch_shapes=[pltpu.VMEM((20, TILE, TILE), KIND)],
        compiler_params=pltpu.CompilerParams(vmem_limit_bytes=20 * MIB),
        cost_estimate=pl.CostEstimate(flops=50 * TILE**3, bytes_accessed=0, transcendentals=0),
    )(core, thresh, far, near, tiles)


def on_device(adj_diag, adj_right, alive_diag, alive_right, truss_k):
    count = lax.axis_size(ROWS)
    core = lax.axis_index("core")
    thresh = truss_k - 2
    within = adj_diag & alive_diag
    across = adj_right & alive_right
    near = lax.ppermute(
        jnp.where(core == 0, within, across),
        ROWS,
        [(i, (i + 2 if i % 2 else i - 2) % count) for i in range(count)],
    )
    chip = lax.all_gather(jnp.concatenate([within, across], axis=0), "core", tiled=True)
    far = lax.ppermute(
        jnp.where(core == 0, chip[: 3 * WORDS], chip[WORDS:]),
        ROWS,
        [(i, (i + 1 if i % 2 else i - 1) % count) for i in range(count)],
    )
    support, removed = peel(core.reshape(1), thresh, far, near, chip_tiles(thresh, chip))
    removed = jnp.sum(lax.all_to_all(removed, FIRST, 0, 0), axis=0, keepdims=True)
    removed = jnp.broadcast_to(removed, (32, 1, 128))
    removed = jnp.sum(lax.all_to_all(removed, SECOND, 0, 0), axis=(0, 1))
    return (support, removed[:ITERS])


def solution(mesh):
    split = Mesh(mesh.devices.reshape(8, 8, 4, 2), ROWS)
    placed = (P(ROWS, None), P(ROWS, None), P(ROWS, None), P(ROWS, None), P())
    return jax.shard_map(
        on_device, mesh=split, in_specs=placed, out_specs=(P(ROWS, None), P()), check_vma=False
    )
```

```python
import functools

import jax
import jax.numpy as jnp
from jax import lax
from jax.experimental import pallas as pl
from jax.experimental.pallas import tpu as pltpu
from jax.sharding import Mesh
from jax.sharding import PartitionSpec as P


ITERS = 3
TILE = 512
HALF = TILE // 2
WORDS = TILE // 32
SIDE = 128
ROWS = ("z", "y", "x", "core")
FIRST = ("y", "core")
SECOND = ("z", "x")
KIND = jnp.float8_e4m3fn
WIDE = jnp.bfloat16
MIB = 1024 * 1024


def unpack(words):
    rows, width = words.shape
    shifts = lax.broadcasted_iota(jnp.int32, (rows, 32, width), 1)
    spread = jnp.broadcast_to(words[:, None, :], (rows, 32, width))
    return ((spread >> shifts) & 1).reshape(rows * 32, width).astype(jnp.float32)


def fill_within(words, ref):
    row_ids = lax.broadcasted_iota(jnp.int32, (SIDE, SIDE), 0)
    col_ids = lax.broadcasted_iota(jnp.int32, (SIDE, SIDE), 1)
    for at in range(0, TILE, SIDE):
        stripe = unpack(words[at // 32 : (at + SIDE) // 32, at:])
        corner = jnp.where(col_ids > row_ids, stripe[:, :SIDE], 0.0)
        flipped = corner.astype(KIND).T.astype(jnp.float32)
        ref[at : at + SIDE, at : at + SIDE] = (corner + flipped).astype(KIND)
        if at + SIDE < TILE:
            rest = stripe[:, SIDE:].astype(KIND)
            ref[at : at + SIDE, at + SIDE :] = rest
            ref[at + SIDE :, at : at + SIDE] = rest.T


def fill_across(words, ref, ref_t):
    tile = unpack(words).astype(KIND)
    ref[...] = tile
    ref_t[...] = tile.T


def times(lhs, rhs):
    return jnp.dot(lhs, rhs, preferred_element_type=jnp.float32)


def inside(left, left_t, here, right, right_t, rows, cols):
    return (
        times(left_t[rows, :], left[:, cols])
        + times(here[rows, :], here[:, cols])
        + times(right[rows, :], right_t[:, cols])
    )


def between(left, here, right, rows):
    return times(left[rows, :], here[...]) + times(here[rows, :], right[...])


def keep(counts, old, thresh):
    return jnp.where(counts.astype(WIDE) >= thresh, old.astype(WIDE), jnp.zeros((), WIDE)).astype(KIND)


TOP, LOW = slice(0, HALF), slice(HALF, TILE)
ALL = slice(0, TILE)


def peel_within(left, left_t, here, right, right_t, thresh, new):
    kept = keep(inside(left, left_t, here, right, right_t, TOP, ALL), here[TOP, :], thresh)
    new[TOP, :] = kept
    new[LOW, TOP] = kept[:, HALF:].T
    new[LOW, LOW] = keep(inside(left, left_t, here, right, right_t, LOW, LOW), here[LOW, LOW], thresh)


def peel_across(left, here, right, thresh, new, new_t):
    for rows in (TOP, LOW):
        kept = keep(between(left, here, right, rows), here[rows, :], thresh)
        new[rows, :] = kept
        new_t[:, rows] = kept.T


def chip_kernel(thresh_ref, chip_ref, tiles_ref):
    thresh = thresh_ref[0].astype(jnp.float32).astype(WIDE)
    w0, a0, a0_t, w1, a1, a1_t, new_a0, new_a0_t, new_w1 = (tiles_ref.at[i] for i in range(9))
    fill_within(chip_ref[:WORDS, :], w0)
    fill_across(chip_ref[WORDS : 2 * WORDS, :], a0, a0_t)
    fill_within(chip_ref[2 * WORDS : 3 * WORDS, :], w1)
    fill_across(chip_ref[3 * WORDS :, :], a1, a1_t)
    peel_across(w0, a0, w1, thresh, new_a0, new_a0_t)
    peel_within(a0, a0_t, w1, a1, a1_t, thresh, new_w1)


def edges(ref):
    tile = ref[...].astype(WIDE)
    parts = [tile[at : at + 32, :] for at in range(0, TILE, 32)]
    while len(parts) > 1:
        parts = [parts[i] + parts[i + 1] for i in range(0, len(parts), 2)]
    return parts[0].astype(jnp.float32)


def chip_levels(chip_ref, core):
    w0, a0, a0_t, w1, a1, a1_t, new_a0, new_a0_t, new_w1 = (chip_ref.at[i] for i in range(9))
    at = 3 - 2 * core
    start = {at: (w0,), at + 1: (a0, a0_t), at + 2: (w1,), at + 3: (a1, a1_t)}
    return start, {at + 1: (new_a0, new_a0_t), at + 2: (new_w1,)}


def fresh_tiles(pool):
    slots = iter(range(pool.shape[0]))
    return lambda index: tuple(pool.at[next(slots)] for _ in range(2 - index % 2))


def fill(words, index, tile):
    (fill_within if index % 2 else fill_across)(words, *tile)


def advance(now, index, thresh, tile):
    left, here, right = now[index - 1], now[index], now[index + 1]
    if index % 2:
        peel_within(*left, *here, *right, thresh, *tile)
    else:
        peel_across(left[0], here[0], right[0], thresh, *tile)
    return tile


def finish(now, index, level, out_ref):
    left, here, right = now[index - 1], now[index], now[index + 1]
    cols = slice((index - 3) * TILE, (index - 2) * TILE)
    last = jnp.zeros((8, TILE), jnp.float32)
    for rows in (TOP, LOW):
        if index % 2:
            counts = inside(*left, *here, *right, rows, ALL)
        else:
            counts = between(left[0], here[0], right[0], rows)
        kept = jnp.where(counts >= level, here[0][rows, :].astype(jnp.float32), 0.0)
        out_ref[rows, cols] = counts * kept
        last = last + jnp.sum(kept.reshape(HALF // 8, 8, TILE), axis=0)
    return jnp.sum(last) * (0.5 if index % 2 else 1.0)


def on_core(core_ref, body):
    for core in range(2):
        pl.when(core_ref[0] == core)(functools.partial(body, core))


def main_kernel(core_ref, thresh_ref, far_ref, chip_ref, out_ref, mids_ref, sums_ref, pool):
    def body(core):
        level = thresh_ref[0].astype(jnp.float32)
        thresh = level.astype(WIDE)
        fresh = fresh_tiles(pool)
        start, once = chip_levels(chip_ref, core)
        own = {3: (mids_ref.at[0],), 4: (mids_ref.at[1], mids_ref.at[2])}
        for slot in range(3):
            index = slot + 5 * core
            start[index] = fresh(index)
            fill(far_ref[slot * WORDS : (slot + 1) * WORDS, :], index, start[index])
        for index in range(1 + core, 6 + core):
            if index not in once:
                once[index] = advance(start, index, thresh, fresh(index))
        twice = {}
        for index in range(2 + core, 5 + core):
            twice[index] = advance(once, index, thresh, own[index] if index in own else fresh(index))
        total = [jnp.sum(edges(now[3][0]) * 0.5 + edges(now[4][0])) for now in (start, once, twice)]
        total.append(finish(twice, 3 + core, level, out_ref))
        lane = lax.broadcasted_iota(jnp.int32, sums_ref.shape, 1)
        sums = jnp.zeros(sums_ref.shape, jnp.float32)
        for step in range(ITERS):
            sums = jnp.where(lane == step, total[step] - total[step + 1], sums)
        sums_ref[...] = sums

    on_core(core_ref, body)


def edge_kernel(core_ref, thresh_ref, near_ref, chip_ref, mids_ref, sums_ref, _, out_ref, count_ref, pool):
    def body(core):
        level = thresh_ref[0].astype(jnp.float32)
        thresh = level.astype(WIDE)
        fresh = fresh_tiles(pool)
        start, once = chip_levels(chip_ref, core)
        twice = {3: (mids_ref.at[0],), 4: (mids_ref.at[1], mids_ref.at[2])}
        step = 1 if core else -1
        index = 0 if core else 7
        start[index] = fresh(index)
        fill(near_ref[...], index, start[index])
        index += step
        once[index] = advance(start, index, thresh, fresh(index))
        index += step
        twice[index] = advance(once, index, thresh, fresh(index))
        last = finish(twice, index + step, level, out_ref)
        sums = jnp.broadcast_to(sums_ref[:1, :][:, None, :], count_ref.shape)
        lane = lax.broadcasted_iota(jnp.int32, count_ref.shape, 2)
        count_ref[...] = jnp.where(lane == ITERS - 1, sums - last, sums).astype(jnp.int32)

    on_core(core_ref, body)


VMEM = pl.BlockSpec(memory_space=pltpu.VMEM)
SMEM = pl.BlockSpec(memory_space=pltpu.SMEM)


def chip_tiles(thresh, chip):
    return pl.pallas_call(
        chip_kernel,
        out_shape=jax.ShapeDtypeStruct((9, TILE, TILE), KIND),
        in_specs=[SMEM, VMEM],
        out_specs=VMEM,
        compiler_params=pltpu.CompilerParams(vmem_limit_bytes=8 * MIB),
        cost_estimate=pl.CostEstimate(flops=10 * TILE**3, bytes_accessed=0, transcendentals=0),
    )(thresh, chip)


def main_part(core, thresh, far, tiles):
    return pl.pallas_call(
        main_kernel,
        out_shape=(
            pltpu.VMEM((TILE, 2 * TILE), jnp.float32),
            pltpu.VMEM((3, TILE, TILE), KIND),
            pltpu.VMEM((8, 128), jnp.float32),
        ),
        in_specs=[SMEM, SMEM, VMEM, VMEM],
        out_specs=(VMEM, VMEM, VMEM),
        scratch_shapes=[pltpu.VMEM((12, TILE, TILE), KIND)],
        compiler_params=pltpu.CompilerParams(vmem_limit_bytes=16 * MIB),
        cost_estimate=pl.CostEstimate(flops=36 * TILE**3, bytes_accessed=0, transcendentals=0),
    )(core, thresh, far, tiles)


def edge_part(core, thresh, near, tiles, mids, sums, support):
    return pl.pallas_call(
        edge_kernel,
        out_shape=(
            pltpu.VMEM((TILE, 2 * TILE), jnp.float32),
            pltpu.VMEM((16, 1, 128), jnp.int32),
        ),
        in_specs=[SMEM, SMEM, VMEM, VMEM, VMEM, VMEM, VMEM],
        out_specs=(VMEM, VMEM),
        input_output_aliases={6: 0},
        scratch_shapes=[pltpu.VMEM((6, TILE, TILE), KIND)],
        compiler_params=pltpu.CompilerParams(vmem_limit_bytes=12 * MIB),
        cost_estimate=pl.CostEstimate(flops=14 * TILE**3, bytes_accessed=0, transcendentals=0),
    )(core, thresh, near, tiles, mids, sums, support)


def on_device(adj_diag, adj_right, alive_diag, alive_right, truss_k):
    count = lax.axis_size(ROWS)
    core = lax.axis_index("core")
    thresh = truss_k - 2
    within = adj_diag & alive_diag
    across = adj_right & alive_right
    chip = lax.all_gather(jnp.concatenate([within, across], axis=0), "core", tiled=True)
    far = lax.ppermute(
        jnp.where(core == 0, chip[: 3 * WORDS], chip[WORDS:]),
        ROWS,
        [(i, (i + 1 if i % 2 else i - 1) % count) for i in range(count)],
    )
    near = lax.ppermute(
        jnp.where(core == 0, within, across),
        ROWS,
        [(i, (i + 2 if i % 2 else i - 2) % count) for i in range(count)],
    )
    core = core.reshape(1)
    tiles = chip_tiles(thresh, chip)
    support, mids, sums = main_part(core, thresh, far, tiles)
    support, removed = edge_part(core, thresh, near, tiles, mids, sums, support)
    removed = jnp.sum(lax.all_to_all(removed, FIRST, 0, 0), axis=0, keepdims=True)
    removed = jnp.broadcast_to(removed, (32, 1, 128))
    removed = jnp.sum(lax.all_to_all(removed, SECOND, 0, 0), axis=(0, 1))
    return (support, removed[:ITERS])


def solution(mesh):
    split = Mesh(mesh.devices.reshape(8, 8, 4, 2), ROWS)
    placed = (P(ROWS, None), P(ROWS, None), P(ROWS, None), P(ROWS, None), P())
    return jax.shard_map(
        on_device, mesh=split, in_specs=placed, out_specs=(P(ROWS, None), P()), check_vma=False
    )
```

```python
import functools
import math

import jax
import jax.numpy as jnp
import numpy as np
from jax import lax
from jax.experimental import pallas as pl
from jax.experimental.pallas import tpu as pltpu
from jax.sharding import Mesh
from jax.sharding import PartitionSpec as P


ITERS = 3
TILE = 512
HALF = TILE // 2
WORDS = TILE // 32
SIDE = 128
ROWS = ("z", "y", "x", "core")
SIZES = (8, 8, 4, 2)
MIDDLE = (6, 6, 2, 1)
KIND = jnp.float8_e4m3fn
WIDE = jnp.bfloat16
MIB = 1024 * 1024


def unpack(words):
    rows, width = words.shape
    shifts = lax.broadcasted_iota(jnp.int32, (rows, 32, width), 1)
    spread = jnp.broadcast_to(words[:, None, :], (rows, 32, width))
    return ((spread >> shifts) & 1).reshape(rows * 32, width).astype(jnp.float32)


def fill_within(words, ref):
    row_ids = lax.broadcasted_iota(jnp.int32, (SIDE, SIDE), 0)
    col_ids = lax.broadcasted_iota(jnp.int32, (SIDE, SIDE), 1)
    for at in range(0, TILE, SIDE):
        stripe = unpack(words[at // 32 : (at + SIDE) // 32, at:])
        corner = jnp.where(col_ids > row_ids, stripe[:, :SIDE], 0.0)
        flipped = corner.astype(KIND).T.astype(jnp.float32)
        ref[at : at + SIDE, at : at + SIDE] = (corner + flipped).astype(KIND)
        if at + SIDE < TILE:
            rest = stripe[:, SIDE:].astype(KIND)
            ref[at : at + SIDE, at + SIDE :] = rest
            ref[at + SIDE :, at : at + SIDE] = rest.T


def fill_across(words, ref, ref_t):
    tile = unpack(words).astype(KIND)
    ref[...] = tile
    ref_t[...] = tile.T


def times(lhs, rhs):
    return jnp.dot(lhs, rhs, preferred_element_type=jnp.float32)


def inside(left, left_t, here, right, right_t, rows, cols):
    return (
        times(left_t[rows, :], left[:, cols])
        + times(here[rows, :], here[:, cols])
        + times(right[rows, :], right_t[:, cols])
    )


def between(left, here, right, rows):
    return times(left[rows, :], here[...]) + times(here[rows, :], right[...])


def keep(counts, old, thresh):
    return jnp.where(counts.astype(WIDE) >= thresh, old.astype(WIDE), jnp.zeros((), WIDE)).astype(KIND)


TOP, LOW = slice(0, HALF), slice(HALF, TILE)
ALL = slice(0, TILE)


def peel_within(left, left_t, here, right, right_t, thresh, new):
    kept = keep(inside(left, left_t, here, right, right_t, TOP, ALL), here[TOP, :], thresh)
    new[TOP, :] = kept
    new[LOW, TOP] = kept[:, HALF:].T
    new[LOW, LOW] = keep(inside(left, left_t, here, right, right_t, LOW, LOW), here[LOW, LOW], thresh)


def peel_across(left, here, right, thresh, new, new_t):
    for rows in (TOP, LOW):
        kept = keep(between(left, here, right, rows), here[rows, :], thresh)
        new[rows, :] = kept
        new_t[:, rows] = kept.T


def chip_kernel(thresh_ref, chip_ref, tiles_ref):
    thresh = thresh_ref[0].astype(jnp.float32).astype(WIDE)
    w0, a0, a0_t, w1, a1, a1_t, new_a0, new_a0_t, new_w1 = (tiles_ref.at[i] for i in range(9))
    fill_within(chip_ref[:WORDS, :], w0)
    fill_across(chip_ref[WORDS : 2 * WORDS, :], a0, a0_t)
    fill_within(chip_ref[2 * WORDS : 3 * WORDS, :], w1)
    fill_across(chip_ref[3 * WORDS :, :], a1, a1_t)
    peel_across(w0, a0, w1, thresh, new_a0, new_a0_t)
    peel_within(a0, a0_t, w1, a1, a1_t, thresh, new_w1)


def edges(ref):
    tile = ref[...].astype(WIDE)
    parts = [tile[at : at + 32, :] for at in range(0, TILE, 32)]
    while len(parts) > 1:
        parts = [parts[i] + parts[i + 1] for i in range(0, len(parts), 2)]
    return parts[0].astype(jnp.float32)


def chip_levels(chip_ref, core):
    w0, a0, a0_t, w1, a1, a1_t, new_a0, new_a0_t, new_w1 = (chip_ref.at[i] for i in range(9))
    at = 3 - 2 * core
    start = {at: (w0,), at + 1: (a0, a0_t), at + 2: (w1,), at + 3: (a1, a1_t)}
    return start, {at + 1: (new_a0, new_a0_t), at + 2: (new_w1,)}


def fresh_tiles(pool):
    slots = iter(range(pool.shape[0]))
    return lambda index: tuple(pool.at[next(slots)] for _ in range(2 - index % 2))


def fill(words, index, tile):
    (fill_within if index % 2 else fill_across)(words, *tile)


def advance(now, index, thresh, tile):
    left, here, right = now[index - 1], now[index], now[index + 1]
    if index % 2:
        peel_within(*left, *here, *right, thresh, *tile)
    else:
        peel_across(left[0], here[0], right[0], thresh, *tile)
    return tile


def finish(now, index, level, out_ref):
    left, here, right = now[index - 1], now[index], now[index + 1]
    cols = slice((index - 3) * TILE, (index - 2) * TILE)
    last = jnp.zeros((8, TILE), jnp.float32)
    for rows in (TOP, LOW):
        if index % 2:
            counts = inside(*left, *here, *right, rows, ALL)
        else:
            counts = between(left[0], here[0], right[0], rows)
        kept = jnp.where(counts >= level, here[0][rows, :].astype(jnp.float32), 0.0)
        out_ref[rows, cols] = counts * kept
        last = last + jnp.sum(kept.reshape(HALF // 8, 8, TILE), axis=0)
    return jnp.sum(last) * (0.5 if index % 2 else 1.0)


def on_core(core_ref, body):
    for core in range(2):
        pl.when(core_ref[0] == core)(functools.partial(body, core))


def main_kernel(core_ref, thresh_ref, far_ref, chip_ref, out_ref, mids_ref, sums_ref, pool):
    def body(core):
        level = thresh_ref[0].astype(jnp.float32)
        thresh = level.astype(WIDE)
        fresh = fresh_tiles(pool)
        start, once = chip_levels(chip_ref, core)
        own = {3: (mids_ref.at[0],), 4: (mids_ref.at[1], mids_ref.at[2])}
        for slot in range(3):
            index = slot + 5 * core
            start[index] = fresh(index)
            fill(far_ref[slot * WORDS : (slot + 1) * WORDS, :], index, start[index])
        for index in range(1 + core, 6 + core):
            if index not in once:
                once[index] = advance(start, index, thresh, fresh(index))
        twice = {}
        for index in range(2 + core, 5 + core):
            twice[index] = advance(once, index, thresh, own[index] if index in own else fresh(index))
        total = [jnp.sum(edges(now[3][0]) * 0.5 + edges(now[4][0])) for now in (start, once, twice)]
        total.append(finish(twice, 3 + core, level, out_ref))
        lane = lax.broadcasted_iota(jnp.int32, sums_ref.shape, 1)
        sums = jnp.zeros(sums_ref.shape, jnp.float32)
        for step in range(ITERS):
            sums = jnp.where(lane == step, total[step] - total[step + 1], sums)
        sums_ref[...] = sums

    on_core(core_ref, body)


def edge_kernel(core_ref, thresh_ref, near_ref, chip_ref, mids_ref, sums_ref, _, out_ref, count_ref, pool):
    def body(core):
        level = thresh_ref[0].astype(jnp.float32)
        thresh = level.astype(WIDE)
        fresh = fresh_tiles(pool)
        start, once = chip_levels(chip_ref, core)
        twice = {3: (mids_ref.at[0],), 4: (mids_ref.at[1], mids_ref.at[2])}
        step = 1 if core else -1
        index = 0 if core else 7
        start[index] = fresh(index)
        fill(near_ref[...], index, start[index])
        index += step
        once[index] = advance(start, index, thresh, fresh(index))
        index += step
        twice[index] = advance(once, index, thresh, fresh(index))
        last = finish(twice, index + step, level, out_ref)
        sums = jnp.broadcast_to(sums_ref[:1, :][:, None, :], count_ref.shape)
        lane = lax.broadcasted_iota(jnp.int32, count_ref.shape, 2)
        count_ref[...] = jnp.where(lane == ITERS - 1, sums - last, sums).astype(jnp.int32)

    on_core(core_ref, body)


VMEM = pl.BlockSpec(memory_space=pltpu.VMEM)
SMEM = pl.BlockSpec(memory_space=pltpu.SMEM)


def chip_tiles(thresh, chip):
    return pl.pallas_call(
        chip_kernel,
        out_shape=jax.ShapeDtypeStruct((9, TILE, TILE), KIND),
        in_specs=[SMEM, VMEM],
        out_specs=VMEM,
        compiler_params=pltpu.CompilerParams(vmem_limit_bytes=8 * MIB),
        cost_estimate=pl.CostEstimate(flops=10 * TILE**3, bytes_accessed=0, transcendentals=0),
    )(thresh, chip)


def main_part(core, thresh, far, tiles):
    return pl.pallas_call(
        main_kernel,
        out_shape=(
            pltpu.VMEM((TILE, 2 * TILE), jnp.float32),
            pltpu.VMEM((3, TILE, TILE), KIND),
            pltpu.VMEM((8, 128), jnp.float32),
        ),
        in_specs=[SMEM, SMEM, VMEM, VMEM],
        out_specs=(VMEM, VMEM, VMEM),
        scratch_shapes=[pltpu.VMEM((12, TILE, TILE), KIND)],
        compiler_params=pltpu.CompilerParams(vmem_limit_bytes=16 * MIB),
        cost_estimate=pl.CostEstimate(flops=36 * TILE**3, bytes_accessed=0, transcendentals=0),
    )(core, thresh, far, tiles)


def edge_part(core, thresh, near, tiles, mids, sums, support):
    return pl.pallas_call(
        edge_kernel,
        out_shape=(
            pltpu.VMEM((TILE, 2 * TILE), jnp.float32),
            pltpu.VMEM((16, 1, 128), jnp.int32),
        ),
        in_specs=[SMEM, SMEM, VMEM, VMEM, VMEM, VMEM, VMEM],
        out_specs=(VMEM, VMEM),
        input_output_aliases={6: 0},
        scratch_shapes=[pltpu.VMEM((6, TILE, TILE), KIND)],
        compiler_params=pltpu.CompilerParams(vmem_limit_bytes=12 * MIB),
        cost_estimate=pl.CostEstimate(flops=14 * TILE**3, bytes_accessed=0, transcendentals=0),
    )(core, thresh, near, tiles, mids, sums, support)


def exchange_groups(axes):
    ids = np.arange(math.prod(SIZES)).reshape(SIZES)
    ids = np.roll(ids, [-at for at in MIDDLE], axis=range(4))
    kept = [axis for axis in range(4) if axis not in axes]
    members = math.prod(SIZES[axis] for axis in axes)
    return ids.transpose(kept + list(axes)).reshape(-1, members).tolist()


def exchange(values, axes):
    groups = exchange_groups(axes)
    values = jnp.broadcast_to(values, (len(groups[0]), 1, 128))
    return lax.all_to_all(values, ROWS, 0, 0, axis_index_groups=groups)


def on_device(adj_diag, adj_right, alive_diag, alive_right, truss_k):
    count = lax.axis_size(ROWS)
    core = lax.axis_index("core")
    thresh = truss_k - 2
    within = adj_diag & alive_diag
    across = adj_right & alive_right
    chip = lax.all_gather(jnp.concatenate([within, across], axis=0), "core", tiled=True)
    far = lax.ppermute(
        jnp.where(core == 0, chip[: 3 * WORDS], chip[WORDS:]),
        ROWS,
        [(i, (i + 1 if i % 2 else i - 1) % count) for i in range(count)],
    )
    near = lax.ppermute(
        jnp.where(core == 0, within, across),
        ROWS,
        [(i, (i + 2 if i % 2 else i - 2) % count) for i in range(count)],
    )
    core = core.reshape(1)
    tiles = chip_tiles(thresh, chip)
    support, mids, sums = main_part(core, thresh, far, tiles)
    support, removed = edge_part(core, thresh, near, tiles, mids, sums, support)
    removed = jnp.sum(exchange(removed, (1, 3)), axis=0, keepdims=True)
    removed = jnp.sum(exchange(removed, (0, 2)), axis=(0, 1))
    return (support, removed[:ITERS])


def solution(mesh):
    split = Mesh(mesh.devices.reshape(8, 8, 4, 2), ROWS)
    placed = (P(ROWS, None), P(ROWS, None), P(ROWS, None), P(ROWS, None), P())
    return jax.shard_map(
        on_device, mesh=split, in_specs=placed, out_specs=(P(ROWS, None), P()), check_vma=False
    )
```
